32 devices in a mesh: win: 2 (over core), grp: 16 (over z, y, x).
Axes of the slice: x: 2, y: 2, z: 4, core: 2. Of those that a mesh axis runs over, the one named last changes fastest.
Arguments:
- atom_table: float32 [4, 6, 24576], P('win', None, 'grp'), as said below
- row_blocks: int32 [4, 1024], P('win', 'grp'), may hold values from 0 to 191, as said below
- col_blocks: int32 [4, 1024], P('win', 'grp'), may hold values from 0 to 191, as said below
- lambdas: float32 [4], replicated, may hold values from 0 to 1, as said below
- inverse_temp: float32 [1], replicated, may hold values from 20 to 80
- parity: int32 [1], replicated, may hold values from 0 to 1073741823
- thresholds: int32 [4], replicated, may hold values from 0 to 1073741823
Outputs:
- energies: float32 [4, 3], P('win')
- margins: float32 [4], P('win')
- profile: float32 [4], P('win')
The draws below stay inside these ranges and needn't reach their ends.
Inputs may be any that keep to these rules, and one draw needn't show every extreme that they name: `row_blocks`: the first block of each pair listed on index g of grp lies in that index's share of atoms: blocks g * 12 to (g + 1) * 12 - 1. `col_blocks`: the list of one index of grp names blocks of any one index of grp (itself included) at most 5 times; in each window some index of grp has exactly 5 of its blocks named in every list of that window. `lambdas`: strictly increasing. `atom_table`: field 4 lies in 0.7 to 1.4 and field 5 in 0.6 to 1.4.
All inputs are finite; a program needn't handle non-finite values.
Results may differ from the reference program's by a relative error of at most 0.0003.
Values sent between devices are 32-bit elements; how exact they have to be, the bound alone decides.
No kernel may reach another device: no remote copies, remote signals or barrier semaphores. Data moves between devices by JAX's collectives and lax.ppermute only.
A program may use at most 64 MiB of HBM per device.

```python
import math
import jax
import jax.numpy as jnp
from jax import lax

TILE = 128
BLK_DEV = 12
PB_DEV = 64
WINDOWS = 4
BLOCKS = 192
ATOMS = 24576
PAIRS = 1024
SLOTS = 5


def draw_atom_table(key, part):
    keys = jax.random.split(key, 12)
    regions = BLOCKS // BLK_DEV
    centres = jax.random.uniform(keys[0], (WINDOWS, 3, BLOCKS, 1), minval=-1.5, maxval=1.5)
    radius = jnp.exp(jax.random.uniform(keys[1], (WINDOWS, 1, BLOCKS, 1), minval=jnp.log(0.25), maxval=jnp.log(0.9)))
    offsets = jax.random.normal(keys[2], (WINDOWS, 3, BLOCKS, TILE))
    region_charge = 0.3 + 0.6 * jax.random.normal(keys[3], (WINDOWS, regions))
    block_charge = 0.3 * jax.random.normal(keys[4], (WINDOWS, BLOCKS))
    atom_charge = 0.3 * jax.random.normal(keys[5], (WINDOWS, BLOCKS, TILE))
    coords = (centres + radius * offsets).reshape(WINDOWS, 3, ATOMS)
    charge_block = jnp.repeat(region_charge, BLK_DEV, axis=1) + block_charge
    charge = (charge_block[:, :, None] + atom_charge).reshape(WINDOWS, 1, ATOMS)
    depth_block = jnp.exp(jax.random.uniform(keys[6], (WINDOWS, BLOCKS, 1), minval=jnp.log(0.75), maxval=jnp.log(1.3)))
    depth_atom = jnp.exp(jax.random.uniform(keys[7], (WINDOWS, BLOCKS, TILE), minval=jnp.log(0.935), maxval=jnp.log(1.07)))
    depth_root = (depth_block * depth_atom).reshape(WINDOWS, 1, ATOMS)
    size_block = jax.random.uniform(keys[8], (WINDOWS, BLOCKS, 1), minval=0.65, maxval=1.35)
    size_atom = jax.random.uniform(keys[9], (WINDOWS, BLOCKS, TILE), minval=-0.05, maxval=0.05)
    size_sq = (size_block + size_atom).reshape(WINDOWS, 1, ATOMS)
    return jnp.concatenate([coords, charge, depth_root, size_sq], axis=1).astype(jnp.float32)


def draw_row_blocks(key, part):
    offset = jnp.arange(PAIRS, dtype=jnp.int32) // PB_DEV * BLK_DEV
    picks = jax.random.randint(key, (WINDOWS, PAIRS), 0, BLK_DEV, dtype=jnp.int32)
    return picks + offset[None, :]


def draw_col_blocks(key, part):
    groups = PAIRS // PB_DEV
    pool = jnp.arange(groups * SLOTS, dtype=jnp.int32) // SLOTS
    keys = jax.random.split(jax.random.fold_in(key, 7), 2)
    heavy = jax.random.randint(keys[0], (WINDOWS,), 0, groups, dtype=jnp.int32)
    list_keys = jax.random.split(keys[1], WINDOWS * groups)

    def one_list(list_key, heavy_owner):
        first_key, second_key, third_key = jax.random.split(list_key, 3)
        order = jax.random.permutation(first_key, groups * SLOTS)
        owners = pool[order]
        placed = jnp.argsort((owners != heavy_owner).astype(jnp.int32), stable=True)
        chosen = owners[placed][:PB_DEV]
        chosen = jax.random.permutation(second_key, chosen)
        within = jax.random.randint(third_key, (PB_DEV,), 0, BLK_DEV, dtype=jnp.int32)
        return (chosen * BLK_DEV + within).astype(jnp.int32)
    heavy_rows = jnp.repeat(heavy, groups)
    lists = jax.vmap(one_list)(list_keys, heavy_rows)
    return lists.reshape(WINDOWS, PAIRS).astype(jnp.int32)


def draw_lambdas(key, part):
    keys = jax.random.split(jax.random.fold_in(key, 11), 3)
    increments = jax.random.uniform(keys[0], (WINDOWS,), minval=0.5, maxval=1.5)
    start = jax.random.uniform(keys[1], (), minval=0.0, maxval=0.25)
    finish = jax.random.uniform(keys[2], (), minval=0.75, maxval=1.0)
    running = jnp.cumsum(increments)
    unit = (running - running[0]) / (running[-1] - running[0])
    return (start + (finish - start) * unit).astype(jnp.float32)


def plant(drawn, key, least, largest):
    extent = drawn.shape
    place = [jax.random.randint(jax.random.fold_in(key, axis), (), 0, extent[axis]) for axis in range(len(extent))]
    drawn = drawn.at[tuple(place)].set(least)
    longest = extent.index(max(extent))
    place[longest] = (place[longest] + 1) % extent[longest]
    return drawn.at[tuple(place)].set(largest)


def setup_inputs(seed: int = 0) -> dict:
    seeds = jax.random.split(jax.random.key(seed), 8)
    return {
        "atom_table": draw_atom_table(jax.random.fold_in(seeds[7], 71), 0),
        "row_blocks": draw_row_blocks(jax.random.fold_in(seeds[7], 71), 0),
        "col_blocks": draw_col_blocks(jax.random.fold_in(seeds[7], 71), 0),
        "lambdas": draw_lambdas(jax.random.fold_in(seeds[7], 71), 0),
        "inverse_temp": jnp.clip(jnp.exp(jax.random.uniform(seeds[4], (1,), jnp.float32, math.log(20.0), math.log(80.0))), 20.0, 80.0),
        "parity": jax.random.randint(seeds[5], (1,), 0, 1073741824).astype(jnp.int32),
        "thresholds": plant(jax.random.randint(seeds[6], (WINDOWS,), 0, 1073741824), jax.random.fold_in(seeds[6], 1), 0, 1073741823).astype(jnp.int32),
    }


tiles_per_step = 16

def pair_energy(row_data, col_data, same_block, lambda_set):
    delta_x = row_data[0][:, :, None] - col_data[0][:, None, :]
    delta_y = row_data[1][:, :, None] - col_data[1][:, None, :]
    delta_z = row_data[2][:, :, None] - col_data[2][:, None, :]
    distance = delta_x * delta_x + delta_y * delta_y + delta_z * delta_z
    charge_pair = row_data[3][:, :, None] * col_data[3][:, None, :]
    well_depth = 4.0 * row_data[4][:, :, None] * col_data[4][:, None, :]
    size_pair = row_data[5][:, :, None] * col_data[5][:, None, :]
    scaled = distance / size_pair
    scaled_cube = scaled * scaled * scaled
    width_tile = distance.shape[-1]
    diagonal = (lax.broadcasted_iota(jnp.int32, (width_tile, width_tile), 0) == lax.broadcasted_iota(jnp.int32, (width_tile, width_tile), 1)).astype(jnp.float32)
    keep_mask = 1.0 - same_block[:, None, None] * diagonal[None]
    totals = []
    for number in range(3):
        lam_now = lambda_set[number]
        softened = 1.0 - 0.5 * lam_now + scaled_cube
        inverse = 1.0 / softened
        dispersion = well_depth * (inverse * inverse - inverse)
        coulomb = charge_pair * lax.rsqrt(distance + 2.0 - lam_now)
        totals.append(lam_now * jnp.sum(keep_mask * (dispersion + coulomb)))
    return jnp.stack(totals)

def window_sums(table, row_ids, col_ids, lambda_set):
    blocks = table.reshape(table.shape[0], -1, TILE)
    row_all = jnp.take(blocks, row_ids, axis=1)
    col_all = jnp.take(blocks, col_ids, axis=1)
    same_all = (row_ids == col_ids).astype(jnp.float32)
    count = row_ids.shape[0] // tiles_per_step

    def advance(number, total):
        start = number * tiles_per_step
        row_part = lax.dynamic_slice_in_dim(row_all, start, tiles_per_step, 1)
        col_part = lax.dynamic_slice_in_dim(col_all, start, tiles_per_step, 1)
        same_part = lax.dynamic_slice_in_dim(same_all, start, tiles_per_step, 0)
        return total + pair_energy(row_part, col_part, same_part, lambda_set)
    return lax.fori_loop(0, count, advance, jnp.zeros((3,), jnp.float32))

def reference(atom_table, row_blocks, col_blocks, lambdas, inverse_temp, parity, thresholds):
    windows = lambdas.shape[0]
    window = jnp.arange(windows, dtype=jnp.int32)
    below = jnp.clip(window - 1, 0, windows - 1)
    above = jnp.clip(window + 1, 0, windows - 1)
    lambda_sets = jnp.stack([lambdas[below], lambdas, lambdas[above]], axis=1)
    sums = lax.map(lambda pack: window_sums(pack[0], pack[1], pack[2], pack[3]), (atom_table, row_blocks, col_blocks, lambda_sets))
    energies = sums / (row_blocks.shape[1] * TILE * TILE)
    d_plus = energies[:, 2] - energies[:, 1]
    d_minus = energies[:, 0] - energies[:, 1]
    profile = jnp.concatenate([jnp.zeros((1,), jnp.float32), jnp.cumsum(d_plus)[:-1]])
    lower_win = jnp.where(jnp.remainder(window - parity[0], 2) == 0, window, window - 1)
    upper_win = lower_win + 1
    has_partner = (lower_win >= 0) & (upper_win < windows)
    lower_safe = jnp.clip(lower_win, 0, windows - 1)
    upper_safe = jnp.clip(upper_win, 0, windows - 1)
    change = d_plus[lower_safe] + d_minus[upper_safe]
    offset_draw = jnp.remainder(thresholds[lower_safe] + parity[0], 1073741824).astype(jnp.int32) + 1
    draw_share = offset_draw.astype(jnp.float32) / 1073741824.0
    margins = jnp.where(has_partner, -jnp.log(draw_share) - inverse_temp[0] * change, 0.0)
    return (energies, margins, profile)
```

```python
import functools

import jax
import jax.numpy as jnp
from jax import lax
from jax.experimental import pallas as pl
from jax.experimental.pallas import tpu as pltpu
from jax.sharding import PartitionSpec as P

TILE = 128
SUB = 8


def split_of(groups):
    outer = 4 if groups % 4 == 0 else 1
    return outer, groups // outer


def is_power(n):
    return n & (n - 1) == 0


def spread_rows(own_ref, rows_scr, window_run, fields, blocks):
    def one(step, carry):
        w, b = step // blocks, lax.rem(step, blocks)
        tile = own_ref[w, pl.ds(b, fields, stride=blocks), :]
        turned = tile.T
        for f in range(fields):
            column = turned[:, f : f + 1]
            if f == 5:
                column = 1.0 / column
            rows_scr[step, f] = jnp.broadcast_to(column, (TILE, TILE))
        return carry

    lax.fori_loop(0, window_run * blocks, one, 0)


def make_plan(place_ref, row_ref, col_ref, near_scr, far_ref, blocks, outer, inner):
    window_run, listed = row_ref.shape
    member = place_ref[0]
    my_plane, my_place = member // inner, lax.rem(member, inner)

    def one_window(w, carry):
        def one(p, counts):
            near, far = counts
            row, col = row_ref[w, p], col_ref[w, p]
            owner = col // blocks
            within = col - owner * blocks
            plane = owner // inner
            place = owner - plane * inner
            turn = lax.rem(my_plane - plane + outer, outer)
            if is_power(inner):
                hop = jnp.bitwise_xor(place, my_place)
            else:
                hop = lax.rem(my_place - place + inner, inner)
            same = jnp.where(row == col, 1, 0)
            local = row - member * blocks
            rest = within * 512 + local * 2 + same
            near_scr[w, near] = turn * 65536 + rest
            far_ref[w, far] = ((hop - 1) * outer + turn) * 65536 + rest
            at_home = jnp.where(hop == 0, 1, 0)
            return near + at_home, far + 1 - at_home

        near, far = lax.fori_loop(0, listed, one, (jnp.int32(0), jnp.int32(0)), unroll=4)
        near_scr[w, listed + 1] = near
        far_ref[w, listed + 1] = far
        return carry

    lax.fori_loop(0, window_run, one_window, 0)


def add_pairs(windows, first_window, lam_ref, list_ref, rows_scr, all_ref, out_ref, with_self):
    window_run = list_ref.shape[0]
    listed = list_ref.shape[1] - 2
    blocks = rows_scr.shape[0] // window_run
    zero = jnp.zeros((SUB, TILE), jnp.float32)

    def evaluate(w, lams):
        count = len(lams)
        softs = [1.0 - 0.5 * lam for lam in lams]
        shifts = [2.0 - lam for lam in lams]

        def block(p, carry):
            packed = list_ref[w, p]
            source = packed // 65536
            within = (packed // 512) & 127
            slot = w * blocks + ((packed // 2) & 255)

            def field(f):
                line = all_ref[source, w, pl.ds(f * blocks + within, 1), :]
                return jnp.broadcast_to(line, (SUB, TILE))

            x, y, z, q, e = (field(f) for f in range(5))
            inv_size = 1.0 / field(5)
            depth = [zero] * count
            charge = [zero] * count
            for r in range(TILE // SUB):
                rows = pl.ds(r * SUB, SUB)
                dx = rows_scr[slot, 0, rows, :] - x
                dy = rows_scr[slot, 1, rows, :] - y
                dz = rows_scr[slot, 2, rows, :] - z
                row_q = rows_scr[slot, 3, rows, :]
                row_e = rows_scr[slot, 4, rows, :]
                r2 = dx * dx + dy * dy + dz * dz
                scaled = r2 * (rows_scr[slot, 5, rows, :] * inv_size)
                cube = scaled * scaled * scaled
                for k in range(count):
                    inverse = 1.0 / (softs[k] + cube)
                    depth[k] = depth[k] + (inverse * inverse - inverse) * row_e
                    charge[k] = charge[k] + lax.rsqrt(r2 + shifts[k]) * row_q
            totals = tuple(
                carry[k] + (4.0 * e) * depth[k] + q * charge[k] for k in range(count)
            )
            if not with_self:
                return totals
            same = (packed & 1).astype(jnp.float32)
            return totals + (carry[count] + same * (e * e), carry[count + 1] + same * (q * q))

        init = (zero,) * (count + 2 * with_self)
        totals = lax.fori_loop(0, list_ref[w, listed + 1], block, init)
        sums = []
        for k in range(count):
            total = totals[k]
            if with_self:
                inverse = 1.0 / (zero + softs[k])
                itself = 4.0 * (inverse * inverse - inverse) * totals[count]
                itself = itself + lax.rsqrt(zero + shifts[k]) * totals[count + 1]
                total = total - itself * (1.0 / SUB)
            sums.append(lams[k] * jnp.sum(total))
        return sums

    def place(window, values):
        shape = out_ref.shape[-2:]
        at_row = lax.broadcasted_iota(jnp.int32, shape, 0) == window
        lane = lax.broadcasted_iota(jnp.int32, shape, 1)
        now = jnp.zeros(shape, jnp.float32)
        for k, value in enumerate(values):
            now = jnp.where(at_row & (lane == k), value, now)
        if len(out_ref.shape) == 3:
            now = jnp.broadcast_to(now[None], out_ref.shape)
        out_ref[...] += now

    def one_window(w, carry):
        window = first_window + w
        below = lam_ref[jnp.maximum(window - 1, 0)]
        here = lam_ref[window]
        above = lam_ref[jnp.minimum(window + 1, windows - 1)]
        is_first = window == 0
        at_end = is_first | (window == windows - 1)

        @pl.when(at_end)
        def _():
            mine, other = evaluate(w, [here, jnp.where(is_first, above, below)])
            place(
                window,
                [jnp.where(is_first, mine, other), mine, jnp.where(is_first, other, mine)],
            )

        @pl.when(jnp.logical_not(at_end))
        def _():
            place(window, evaluate(w, [below, here, above]))

        return carry

    lax.fori_loop(0, window_run, one_window, 0)


def near_kernel(
    windows, outer, inner,
    place_ref, lam_ref, row_ref, col_ref, own_ref, column_ref,
    out_ref, far_ref, rows_scr, near_scr,
):
    window_run = row_ref.shape[0]
    fields = rows_scr.shape[1]
    blocks = rows_scr.shape[0] // window_run
    make_plan(place_ref, row_ref, col_ref, near_scr, far_ref, blocks, outer, inner)
    spread_rows(own_ref, rows_scr, window_run, fields, blocks)
    out_ref[...] = jnp.zeros_like(out_ref)
    add_pairs(windows, place_ref[1], lam_ref, near_scr, rows_scr, column_ref, out_ref, True)


def far_kernel(windows, outer, inner, place_ref, lam_ref, far_ref, own_ref, near_ref, *rest):
    sources, (out_ref, rows_scr, all_scr) = rest[:-3], rest[-3:]
    window_run = far_ref.shape[0]
    fields = rows_scr.shape[1]
    blocks = rows_scr.shape[0] // window_run
    for k, source in enumerate(sources):
        all_scr[k * outer : (k + 1) * outer] = source[...]
    spread_rows(own_ref, rows_scr, window_run, fields, blocks)
    out_ref[...] = jnp.broadcast_to(near_ref[...][None], out_ref.shape)
    add_pairs(windows, place_ref[1], lam_ref, far_ref, rows_scr, all_scr, out_ref, False)


def per_device(atom_table, row_blocks, col_blocks, lambdas, inverse_temp, parity, thresholds):
    window_run, fields, atoms = atom_table.shape
    windows = lax.axis_size("win") * window_run
    groups = lax.axis_size("grp")
    outer, inner = split_of(groups)
    listed = row_blocks.shape[1]
    blocks = atoms // TILE
    member = lax.axis_index("grp")
    first_window = lax.axis_index("win") * window_run
    own = atom_table.reshape(window_run, fields * blocks, TILE)

    def from_plane(k):
        pairs = [(i, (i + k * inner) % groups) for i in range(groups)]
        return lax.ppermute(own, "grp", pairs)

    column = jnp.stack([own] + [from_plane(k) for k in range(1, outer)])

    def from_place(k):
        def target(i):
            plane, place = divmod(i, inner)
            return plane * inner + ((place ^ k) if is_power(inner) else (place + k) % inner)

        return lax.ppermute(column, "grp", [(i, target(i)) for i in range(groups)])

    others = [from_place(k) for k in range(1, inner)]
    smem = pl.BlockSpec(memory_space=pltpu.SMEM)
    vmem = pl.BlockSpec(memory_space=pltpu.VMEM)
    place = jnp.stack([member, first_window]).astype(jnp.int32)
    rows_scratch = pltpu.VMEM((window_run * blocks, fields, TILE, TILE), jnp.float32)
    per_pair = 100 * TILE * TILE * listed * window_run
    near, far_list = pl.pallas_call(
        functools.partial(near_kernel, windows, outer, inner),
        out_shape=(
            jax.ShapeDtypeStruct((windows, TILE), jnp.float32),
            jax.ShapeDtypeStruct((window_run, listed + 2), jnp.int32),
        ),
        in_specs=[smem, smem, smem, smem, vmem, vmem],
        out_specs=(vmem, smem),
        scratch_shapes=[rows_scratch, pltpu.SMEM((window_run, listed + 2), jnp.int32)],
        cost_estimate=pl.CostEstimate(
            flops=per_pair // inner, bytes_accessed=0, transcendentals=0
        ),
    )(place, lambdas, row_blocks, col_blocks, own, column)
    if others:
        partial = pl.pallas_call(
            functools.partial(far_kernel, windows, outer, inner),
            out_shape=jax.ShapeDtypeStruct((groups, windows, TILE), jnp.float32),
            in_specs=[smem, smem, smem, vmem, vmem] + [vmem] * len(others),
            out_specs=vmem,
            scratch_shapes=[
                rows_scratch,
                pltpu.VMEM((len(others) * outer,) + own.shape, jnp.float32),
            ],
            cost_estimate=pl.CostEstimate(
                flops=per_pair, bytes_accessed=0, transcendentals=0
            ),
        )(place, lambdas, far_list, own, near, *others)
    else:
        partial = jnp.broadcast_to(near[None], (groups,) + near.shape)
    shared = lax.all_to_all(partial, "grp", split_axis=0, concat_axis=0, tiled=True)
    summed = lax.psum(jnp.sum(shared, axis=0), "win")[:, :3]
    energy = summed / (listed * groups * TILE * TILE)
    up = energy[:, 2] - energy[:, 1]
    down = energy[:, 0] - energy[:, 1]
    window = jnp.arange(windows, dtype=jnp.int32)
    lower = jnp.where(jnp.remainder(window - parity[0], 2) == 0, window, window - 1)
    upper = lower + 1
    has_partner = (lower >= 0) & (upper < windows)
    is_lower = lower == window
    down_next = jnp.concatenate([down[1:], down[:1]])
    up_prev = jnp.concatenate([up[-1:], up[:-1]])
    change = jnp.where(is_lower, up + down_next, up_prev + down)
    drawn = jnp.where(is_lower, thresholds, jnp.concatenate([thresholds[-1:], thresholds[:-1]]))
    share = (jnp.remainder(drawn + parity[0], 1073741824) + 1).astype(jnp.float32) / 1073741824.0
    margins = jnp.where(has_partner, -jnp.log(share) - inverse_temp[0] * change, 0.0)
    earlier = window[None, :] < window[:, None]
    profile = jnp.sum(jnp.where(earlier, up[None, :], 0.0), axis=1)

    def mine(whole):
        return lax.dynamic_slice_in_dim(whole, first_window, window_run, 0)

    return mine(energy), mine(margins), mine(profile)


def solution(mesh):
    return jax.shard_map(
        per_device,
        mesh=mesh,
        in_specs=(P("win", None, "grp"), P("win", "grp"), P("win", "grp"), P(), P(), P(), P()),
        out_specs=(P("win", None), P("win"), P("win")),
        check_vma=False,
    )
```

```python
import functools

import jax
import jax.numpy as jnp
from jax import lax
from jax.experimental import pallas as pl
from jax.experimental.pallas import tpu as pltpu
from jax.sharding import PartitionSpec as P

TILE = 128
SUB = 8


def split_of(groups):
    outer = 4 if groups % 4 == 0 else 1
    return outer, groups // outer


def is_power(n):
    return n & (n - 1) == 0


def spread_rows(own_ref, rows_scr, window_run, fields, blocks):
    def one_window(w, carry):
        turned = own_ref[w].T
        inverse = 1.0 / turned
        for b in range(blocks):
            for f in range(fields):
                at = f * blocks + b
                column = (inverse if f == 5 else turned)[:, at : at + 1]
                rows_scr[w * blocks + b, f] = jnp.broadcast_to(column, (TILE, TILE))
        return carry

    lax.fori_loop(0, window_run, one_window, 0)


def make_plan(place_ref, row_ref, col_ref, near_scr, next_ref, far_ref, blocks, outer, inner):
    window_run, listed = row_ref.shape
    member = place_ref[0]
    my_plane, my_place = member // inner, lax.rem(member, inner)

    def one_window(w, carry):
        def one(p, counts):
            near, after, far = counts
            row, col = row_ref[w, p], col_ref[w, p]
            owner = col // blocks
            within = col - owner * blocks
            plane = owner // inner
            place = owner - plane * inner
            turn = lax.rem(my_plane - plane + outer, outer)
            if is_power(inner):
                hop = jnp.bitwise_xor(place, my_place)
            else:
                hop = lax.rem(my_place - place + inner, inner)
            same = jnp.where(row == col, 1, 0)
            local = row - member * blocks
            rest = within * 512 + local * 2 + same
            near_scr[w, near] = turn * 65536 + rest
            next_ref[w, after] = turn * 65536 + rest
            far_ref[w, far] = ((hop - 2) * outer + turn) * 65536 + rest
            at_home = jnp.where(hop == 0, 1, 0)
            at_next = jnp.where(hop == 1, 1, 0)
            return near + at_home, after + at_next, far + 1 - at_home - at_next

        none = jnp.int32(0)
        near, after, far = lax.fori_loop(0, listed, one, (none, none, none), unroll=4)
        near_scr[w, listed + 1] = near
        next_ref[w, listed + 1] = after
        far_ref[w, listed + 1] = far
        return carry

    lax.fori_loop(0, window_run, one_window, 0)


def add_pairs(windows, first_window, lam_ref, list_ref, rows_scr, all_ref, out_ref, with_self):
    window_run = list_ref.shape[0]
    listed = list_ref.shape[1] - 2
    blocks = rows_scr.shape[0] // window_run
    zero = jnp.zeros((SUB, TILE), jnp.float32)

    def evaluate(w, lams):
        count = len(lams)
        softs = [1.0 - 0.5 * lam for lam in lams]
        shifts = [2.0 - lam for lam in lams]

        def block(p, carry):
            packed = list_ref[w, p]
            source = packed // 65536
            within = (packed // 512) & 127
            slot = w * blocks + ((packed // 2) & 255)

            def field(f):
                line = all_ref[source, w, pl.ds(f * blocks + within, 1), :]
                return jnp.broadcast_to(line, (SUB, TILE))

            x, y, z, q, e = (field(f) for f in range(5))
            inv_size = 1.0 / field(5)
            depth = [zero] * count
            charge = [zero] * count
            for r in range(TILE // SUB):
                rows = pl.ds(r * SUB, SUB)
                dx = rows_scr[slot, 0, rows, :] - x
                dy = rows_scr[slot, 1, rows, :] - y
                dz = rows_scr[slot, 2, rows, :] - z
                row_q = rows_scr[slot, 3, rows, :]
                row_e = rows_scr[slot, 4, rows, :]
                r2 = dx * dx + dy * dy + dz * dz
                scaled = r2 * (rows_scr[slot, 5, rows, :] * inv_size)
                cube = scaled * scaled * scaled
                for k in range(count):
                    inverse = 1.0 / (softs[k] + cube)
                    depth[k] = depth[k] + (inverse * inverse - inverse) * row_e
                    charge[k] = charge[k] + lax.rsqrt(r2 + shifts[k]) * row_q
            totals = tuple(
                carry[k] + (4.0 * e) * depth[k] + q * charge[k] for k in range(count)
            )
            if not with_self:
                return totals
            same = (packed & 1).astype(jnp.float32)
            return totals + (carry[count] + same * (e * e), carry[count + 1] + same * (q * q))

        init = (zero,) * (count + 2 * with_self)
        totals = lax.fori_loop(0, list_ref[w, listed + 1], block, init)
        sums = []
        for k in range(count):
            total = totals[k]
            if with_self:
                inverse = 1.0 / (zero + softs[k])
                itself = 4.0 * (inverse * inverse - inverse) * totals[count]
                itself = itself + lax.rsqrt(zero + shifts[k]) * totals[count + 1]
                total = total - itself * (1.0 / SUB)
            sums.append(lams[k] * jnp.sum(total))
        return sums

    def place(window, values):
        shape = out_ref.shape[-2:]
        at_row = lax.broadcasted_iota(jnp.int32, shape, 0) == window
        lane = lax.broadcasted_iota(jnp.int32, shape, 1)
        now = jnp.zeros(shape, jnp.float32)
        for k, value in enumerate(values):
            now = jnp.where(at_row & (lane == k), value, now)
        if len(out_ref.shape) == 3:
            now = jnp.broadcast_to(now[None], out_ref.shape)
        out_ref[...] += now

    def one_window(w, carry):
        window = first_window + w
        below = lam_ref[jnp.maximum(window - 1, 0)]
        here = lam_ref[window]
        above = lam_ref[jnp.minimum(window + 1, windows - 1)]
        is_first = window == 0
        at_end = is_first | (window == windows - 1)

        @pl.when(at_end)
        def _():
            mine, other = evaluate(w, [here, jnp.where(is_first, above, below)])
            place(
                window,
                [jnp.where(is_first, mine, other), mine, jnp.where(is_first, other, mine)],
            )

        @pl.when(jnp.logical_not(at_end))
        def _():
            place(window, evaluate(w, [below, here, above]))

        return carry

    lax.fori_loop(0, window_run, one_window, 0)


def swap_of(window, windows, parity):
    lower = jnp.where(((window - parity) & 1) == 0, window, window - 1)
    has_partner = (lower >= 0) & (lower + 1 < windows)
    return jnp.clip(lower, 0, windows - 1), has_partner


def near_kernel(
    windows, outer, inner,
    place_ref, lam_ref, parity_ref, drawn_ref, row_ref, col_ref, own_ref, column_ref,
    out_ref, next_ref, far_ref, log_ref, rows_scr, near_scr,
):
    window_run = row_ref.shape[0]
    fields = rows_scr.shape[1]
    blocks = rows_scr.shape[0] // window_run
    make_plan(place_ref, row_ref, col_ref, near_scr, next_ref, far_ref, blocks, outer, inner)
    for w in range(window_run):
        lower, _ = swap_of(place_ref[1] + w, windows, parity_ref[0])
        ticket = ((drawn_ref[lower] + parity_ref[0]) & (2**30 - 1)) + 1
        share = jnp.full((SUB, TILE), ticket, jnp.int32).astype(jnp.float32) / 1073741824.0
        log_ref[w] = jnp.max(-jnp.log(share))
    spread_rows(own_ref, rows_scr, window_run, fields, blocks)
    out_ref[...] = jnp.zeros_like(out_ref)
    add_pairs(windows, place_ref[1], lam_ref, near_scr, rows_scr, column_ref, out_ref, True)


def next_kernel(
    windows, place_ref, lam_ref, next_ref, own_ref, before_ref, source_ref, out_ref, rows_scr
):
    window_run, blocks = next_ref.shape[0], rows_scr.shape[0] // next_ref.shape[0]
    spread_rows(own_ref, rows_scr, window_run, rows_scr.shape[1], blocks)
    out_ref[...] = before_ref[...]
    add_pairs(windows, place_ref[1], lam_ref, next_ref, rows_scr, source_ref, out_ref, False)


def far_kernel(windows, outer, place_ref, lam_ref, far_ref, own_ref, before_ref, *rest):
    sources, (out_ref, rows_scr, all_scr) = rest[:-3], rest[-3:]
    window_run, blocks = far_ref.shape[0], rows_scr.shape[0] // far_ref.shape[0]
    for k, source in enumerate(sources):
        all_scr[k * outer : (k + 1) * outer] = source[...]
    spread_rows(own_ref, rows_scr, window_run, rows_scr.shape[1], blocks)
    out_ref[...] = jnp.broadcast_to(before_ref[...][None], out_ref.shape)
    add_pairs(windows, place_ref[1], lam_ref, far_ref, rows_scr, all_scr, out_ref, False)


def tail_kernel(
    windows, scale, place_ref, parity_ref, temp_ref, log_ref, sums_ref,
    energy_ref, margin_ref, profile_ref,
):
    window_run = energy_ref.shape[0]
    energy = [[sums_ref[w, k] * scale for k in range(3)] for w in range(windows)]
    up = [row[2] - row[1] for row in energy]
    down = [row[0] - row[1] for row in energy]

    def pick(values, index):
        taken = values[0]
        for v in range(1, len(values)):
            taken = jnp.where(index == v, values[v], taken)
        return taken

    before = [jnp.float32(0)]
    for v in range(windows - 1):
        before.append(before[-1] + up[v])
    for w in range(window_run):
        window = place_ref[1] + w
        lower, has_partner = swap_of(window, windows, parity_ref[0])
        change = pick(up, lower) + pick(down, lower + 1)
        margin_ref[w] = jnp.where(has_partner, log_ref[w] - temp_ref[0] * change, 0.0)
        profile_ref[w] = pick(before, window)
        for k in range(3):
            energy_ref[w, k] = pick([row[k] for row in energy], window)


def per_device(atom_table, row_blocks, col_blocks, lambdas, inverse_temp, parity, thresholds):
    window_run, fields, atoms = atom_table.shape
    windows = lax.axis_size("win") * window_run
    groups = lax.axis_size("grp")
    outer, inner = split_of(groups)
    listed = row_blocks.shape[1]
    blocks = atoms // TILE
    member = lax.axis_index("grp")
    first_window = lax.axis_index("win") * window_run
    own = atom_table.reshape(window_run, fields * blocks, TILE)

    def from_plane(k):
        pairs = [(i, (i + k * inner) % groups) for i in range(groups)]
        return lax.ppermute(own, "grp", pairs)

    column = jnp.stack([own] + [from_plane(k) for k in range(1, outer)])

    def from_place(k):
        def target(i):
            plane, place = divmod(i, inner)
            return plane * inner + ((place ^ k) if is_power(inner) else (place + k) % inner)

        return lax.ppermute(column, "grp", [(i, target(i)) for i in range(groups)])

    others = [from_place(k) for k in range(1, inner)]
    smem = pl.BlockSpec(memory_space=pltpu.SMEM)
    vmem = pl.BlockSpec(memory_space=pltpu.VMEM)
    place = jnp.stack([member, first_window]).astype(jnp.int32)
    rows_scratch = pltpu.VMEM((window_run * blocks, fields, TILE, TILE), jnp.float32)
    per_pair = 100 * TILE * TILE * listed * window_run
    plan = jax.ShapeDtypeStruct((window_run, listed + 2), jnp.int32)
    sums = jax.ShapeDtypeStruct((windows, TILE), jnp.float32)

    def cost(part):
        return pl.CostEstimate(flops=per_pair * part // inner, bytes_accessed=0, transcendentals=0)

    done, next_list, far_list, logs = pl.pallas_call(
        functools.partial(near_kernel, windows, outer, inner),
        out_shape=(sums, plan, plan, jax.ShapeDtypeStruct((window_run,), jnp.float32)),
        in_specs=[smem] * 6 + [vmem] * 2,
        out_specs=(vmem, smem, smem, smem),
        scratch_shapes=[rows_scratch, pltpu.SMEM((window_run, listed + 2), jnp.int32)],
        cost_estimate=cost(1),
    )(place, lambdas, parity, thresholds, row_blocks, col_blocks, own, column)
    if inner > 1:
        done = pl.pallas_call(
            functools.partial(next_kernel, windows),
            out_shape=sums,
            in_specs=[smem] * 3 + [vmem] * 3,
            out_specs=vmem,
            scratch_shapes=[rows_scratch],
            cost_estimate=cost(1),
        )(place, lambdas, next_list, own, done, others[0])
    if inner > 2:
        partial = pl.pallas_call(
            functools.partial(far_kernel, windows, outer),
            out_shape=jax.ShapeDtypeStruct((groups, windows, TILE), jnp.float32),
            in_specs=[smem] * 3 + [vmem] * (1 + inner - 1),
            out_specs=vmem,
            scratch_shapes=[
                rows_scratch,
                pltpu.VMEM(((inner - 2) * outer,) + own.shape, jnp.float32),
            ],
            cost_estimate=cost(inner - 2),
        )(place, lambdas, far_list, own, done, *others[1:])
    else:
        partial = jnp.broadcast_to(done[None], (groups,) + done.shape)
    shared = lax.all_to_all(partial, "grp", split_axis=0, concat_axis=0, tiled=True)
    summed = lax.psum(jnp.sum(shared, axis=0), "win")
    scale = 1.0 / (listed * groups * TILE * TILE)
    return pl.pallas_call(
        functools.partial(tail_kernel, windows, scale),
        out_shape=(
            jax.ShapeDtypeStruct((window_run, 3), jnp.float32),
            jax.ShapeDtypeStruct((window_run,), jnp.float32),
            jax.ShapeDtypeStruct((window_run,), jnp.float32),
        ),
        in_specs=[smem] * 5,
        out_specs=(smem, smem, smem),
    )(place, parity, inverse_temp, logs, summed)


def solution(mesh):
    return jax.shard_map(
        per_device,
        mesh=mesh,
        in_specs=(P("win", None, "grp"), P("win", "grp"), P("win", "grp"), P(), P(), P(), P()),
        out_specs=(P("win", None), P("win"), P("win")),
        check_vma=False,
    )
```

```python
import functools

import jax
import jax.numpy as jnp
from jax import lax
from jax.experimental import pallas as pl
from jax.experimental.pallas import tpu as pltpu
from jax.sharding import PartitionSpec as P

TILE = 128
SUB = 8


def split_of(groups):
    outer = 4 if groups % 4 == 0 else 1
    return outer, groups // outer


def is_power(n):
    return n & (n - 1) == 0


def spread_rows(own_ref, rows_scr, window_run, fields, blocks):
    def one_window(w, carry):
        turned = own_ref[w].T
        inverse = 1.0 / turned
        for b in range(blocks):
            for f in range(fields):
                at = f * blocks + b
                column = (inverse if f == 5 else turned)[:, at : at + 1]
                rows_scr[w * blocks + b, f] = jnp.broadcast_to(column, (TILE, TILE))
        return carry

    lax.fori_loop(0, window_run, one_window, 0)


def make_plan(place_ref, row_ref, col_ref, near_scr, far_ref, blocks, outer, inner):
    window_run, listed = row_ref.shape
    member = place_ref[0]
    my_plane, my_place = member // inner, lax.rem(member, inner)

    def one_window(w, carry):
        def one(p, counts):
            near, far = counts
            row, col = row_ref[w, p], col_ref[w, p]
            owner = col // blocks
            within = col - owner * blocks
            plane = owner // inner
            place = owner - plane * inner
            turn = lax.rem(my_plane - plane + outer, outer)
            if is_power(inner):
                hop = jnp.bitwise_xor(place, my_place)
            else:
                hop = lax.rem(my_place - place + inner, inner)
            same = jnp.where(row == col, 1, 0)
            local = row - member * blocks
            rest = within * 512 + local * 2 + same
            near_scr[w, near] = turn * 65536 + rest
            far_ref[w, far] = ((hop - 1) * outer + turn) * 65536 + rest
            at_home = jnp.where(hop == 0, 1, 0)
            return near + at_home, far + 1 - at_home

        none = jnp.int32(0)
        near, far = lax.fori_loop(0, listed, one, (none, none), unroll=4)
        near_scr[w, listed + 1] = near
        far_ref[w, listed + 1] = far
        return carry

    lax.fori_loop(0, window_run, one_window, 0)


def add_pairs(windows, first_window, lam_ref, list_ref, rows_scr, all_ref, out_ref, with_self):
    window_run = list_ref.shape[0]
    listed = list_ref.shape[1] - 2
    blocks = rows_scr.shape[0] // window_run
    zero = jnp.zeros((SUB, TILE), jnp.float32)

    def evaluate(w, lams):
        count = len(lams)
        softs = [1.0 - 0.5 * lam for lam in lams]
        shifts = [2.0 - lam for lam in lams]

        def block(p, carry):
            packed = list_ref[w, p]
            source = packed // 65536
            within = (packed // 512) & 127
            slot = w * blocks + ((packed // 2) & 255)

            def field(f):
                line = all_ref[source, w, pl.ds(f * blocks + within, 1), :]
                return jnp.broadcast_to(line, (SUB, TILE))

            x, y, z, q, e = (field(f) for f in range(5))
            inv_size = 1.0 / field(5)
            depth = [zero] * count
            charge = [zero] * count
            for r in range(TILE // SUB):
                rows = pl.ds(r * SUB, SUB)
                dx = rows_scr[slot, 0, rows, :] - x
                dy = rows_scr[slot, 1, rows, :] - y
                dz = rows_scr[slot, 2, rows, :] - z
                row_q = rows_scr[slot, 3, rows, :]
                row_e = rows_scr[slot, 4, rows, :]
                r2 = dx * dx + dy * dy + dz * dz
                scaled = r2 * (rows_scr[slot, 5, rows, :] * inv_size)
                cube = scaled * scaled * scaled
                for k in range(count):
                    inverse = 1.0 / (softs[k] + cube)
                    depth[k] = depth[k] + (inverse * inverse - inverse) * row_e
                    charge[k] = charge[k] + lax.rsqrt(r2 + shifts[k]) * row_q
            totals = tuple(
                carry[k] + (4.0 * e) * depth[k] + q * charge[k] for k in range(count)
            )
            if not with_self:
                return totals
            same = (packed & 1).astype(jnp.float32)
            return totals + (carry[count] + same * (e * e), carry[count + 1] + same * (q * q))

        init = (zero,) * (count + 2 * with_self)
        totals = lax.fori_loop(0, list_ref[w, listed + 1], block, init)
        sums = []
        for k in range(count):
            total = totals[k]
            if with_self:
                inverse = 1.0 / (zero + softs[k])
                itself = 4.0 * (inverse * inverse - inverse) * totals[count]
                itself = itself + lax.rsqrt(zero + shifts[k]) * totals[count + 1]
                total = total - itself * (1.0 / SUB)
            sums.append(lams[k] * jnp.sum(total))
        return sums

    def place(window, values):
        shape = out_ref.shape[-2:]
        at_row = lax.broadcasted_iota(jnp.int32, shape, 0) == window
        lane = lax.broadcasted_iota(jnp.int32, shape, 1)
        now = jnp.zeros(shape, jnp.float32)
        for k, value in enumerate(values):
            now = jnp.where(at_row & (lane == k), value, now)
        if len(out_ref.shape) == 3:
            now = jnp.broadcast_to(now[None], out_ref.shape)
        out_ref[...] += now

    def one_window(w, carry):
        window = first_window + w
        below = lam_ref[jnp.maximum(window - 1, 0)]
        here = lam_ref[window]
        above = lam_ref[jnp.minimum(window + 1, windows - 1)]
        is_first = window == 0
        at_end = is_first | (window == windows - 1)

        @pl.when(at_end)
        def _():
            mine, other = evaluate(w, [here, jnp.where(is_first, above, below)])
            place(
                window,
                [jnp.where(is_first, mine, other), mine, jnp.where(is_first, other, mine)],
            )

        @pl.when(jnp.logical_not(at_end))
        def _():
            place(window, evaluate(w, [below, here, above]))

        return carry

    lax.fori_loop(0, window_run, one_window, 0)


def swap_of(window, windows, parity):
    lower = jnp.where(((window - parity) & 1) == 0, window, window - 1)
    has_partner = (lower >= 0) & (lower + 1 < windows)
    return jnp.clip(lower, 0, windows - 1), has_partner


def near_kernel(
    windows, outer, inner,
    place_ref, lam_ref, parity_ref, drawn_ref, row_ref, col_ref, own_ref, column_ref,
    out_ref, far_ref, log_ref, rows_scr, near_scr,
):
    window_run = row_ref.shape[0]
    fields = rows_scr.shape[1]
    blocks = rows_scr.shape[0] // window_run
    make_plan(place_ref, row_ref, col_ref, near_scr, far_ref, blocks, outer, inner)
    for w in range(window_run):
        lower, _ = swap_of(place_ref[1] + w, windows, parity_ref[0])
        ticket = ((drawn_ref[lower] + parity_ref[0]) & (2**30 - 1)) + 1
        share = jnp.full((SUB, TILE), ticket, jnp.int32).astype(jnp.float32) / 1073741824.0
        log_ref[w] = jnp.max(-jnp.log(share))
    spread_rows(own_ref, rows_scr, window_run, fields, blocks)
    out_ref[...] = jnp.zeros_like(out_ref)
    add_pairs(windows, place_ref[1], lam_ref, near_scr, rows_scr, column_ref, out_ref, True)


def far_kernel(windows, outer, place_ref, lam_ref, far_ref, own_ref, before_ref, *rest):
    sources, (out_ref, rows_scr, all_scr) = rest[:-3], rest[-3:]
    window_run, blocks = far_ref.shape[0], rows_scr.shape[0] // far_ref.shape[0]
    for k, source in enumerate(sources):
        all_scr[k * outer : (k + 1) * outer] = source[...]
    spread_rows(own_ref, rows_scr, window_run, rows_scr.shape[1], blocks)
    out_ref[...] = jnp.broadcast_to(before_ref[...][None], out_ref.shape)
    add_pairs(windows, place_ref[1], lam_ref, far_ref, rows_scr, all_scr, out_ref, False)


def tail_kernel(
    windows, scale, place_ref, parity_ref, temp_ref, log_ref, sums_ref,
    energy_ref, margin_ref, profile_ref,
):
    window_run = energy_ref.shape[0]
    energy = [[sums_ref[w, k] * scale for k in range(3)] for w in range(windows)]
    up = [row[2] - row[1] for row in energy]
    down = [row[0] - row[1] for row in energy]

    def pick(values, index):
        taken = values[0]
        for v in range(1, len(values)):
            taken = jnp.where(index == v, values[v], taken)
        return taken

    before = [jnp.float32(0)]
    for v in range(windows - 1):
        before.append(before[-1] + up[v])
    for w in range(window_run):
        window = place_ref[1] + w
        lower, has_partner = swap_of(window, windows, parity_ref[0])
        change = pick(up, lower) + pick(down, lower + 1)
        margin_ref[w] = jnp.where(has_partner, log_ref[w] - temp_ref[0] * change, 0.0)
        profile_ref[w] = pick(before, window)
        for k in range(3):
            energy_ref[w, k] = pick([row[k] for row in energy], window)


def per_device(atom_table, row_blocks, col_blocks, lambdas, inverse_temp, parity, thresholds):
    window_run, fields, atoms = atom_table.shape
    windows = lax.axis_size("win") * window_run
    groups = lax.axis_size("grp")
    outer, inner = split_of(groups)
    listed = row_blocks.shape[1]
    blocks = atoms // TILE
    member = lax.axis_index("grp")
    first_window = lax.axis_index("win") * window_run
    own = atom_table.reshape(window_run, fields * blocks, TILE)

    def from_plane(k):
        pairs = [(i, (i + k * inner) % groups) for i in range(groups)]
        return lax.ppermute(own, "grp", pairs)

    column = jnp.stack([own] + [from_plane(k) for k in range(1, outer)])

    def from_place(k):
        def target(i):
            plane, place = divmod(i, inner)
            return plane * inner + ((place ^ k) if is_power(inner) else (place + k) % inner)

        return lax.ppermute(column, "grp", [(i, target(i)) for i in range(groups)])

    others = [from_place(k) for k in range(1, inner)]
    smem = pl.BlockSpec(memory_space=pltpu.SMEM)
    vmem = pl.BlockSpec(memory_space=pltpu.VMEM)
    place = jnp.stack([member, first_window]).astype(jnp.int32)
    rows_scratch = pltpu.VMEM((window_run * blocks, fields, TILE, TILE), jnp.float32)
    per_pair = 100 * TILE * TILE * listed * window_run
    plan = jax.ShapeDtypeStruct((window_run, listed + 2), jnp.int32)
    sums = jax.ShapeDtypeStruct((windows, TILE), jnp.float32)

    def cost(part):
        return pl.CostEstimate(flops=per_pair * part // inner, bytes_accessed=0, transcendentals=0)

    done, far_list, logs = pl.pallas_call(
        functools.partial(near_kernel, windows, outer, inner),
        out_shape=(sums, plan, jax.ShapeDtypeStruct((window_run,), jnp.float32)),
        in_specs=[smem] * 6 + [vmem] * 2,
        out_specs=(vmem, smem, smem),
        scratch_shapes=[rows_scratch, pltpu.SMEM((window_run, listed + 2), jnp.int32)],
        cost_estimate=cost(1),
    )(place, lambdas, parity, thresholds, row_blocks, col_blocks, own, column)
    if inner > 1:
        partial = pl.pallas_call(
            functools.partial(far_kernel, windows, outer),
            out_shape=jax.ShapeDtypeStruct((groups, windows, TILE), jnp.float32),
            in_specs=[smem] * 3 + [vmem] * (1 + inner),
            out_specs=vmem,
            scratch_shapes=[
                rows_scratch,
                pltpu.VMEM(((inner - 1) * outer,) + own.shape, jnp.float32),
            ],
            cost_estimate=cost(inner - 1),
        )(place, lambdas, far_list, own, done, *others)
    else:
        partial = jnp.broadcast_to(done[None], (groups,) + done.shape)
    shared = lax.all_to_all(partial, "grp", split_axis=0, concat_axis=0, tiled=True)
    summed = lax.psum(jnp.sum(shared, axis=0), "win")
    scale = 1.0 / (listed * groups * TILE * TILE)
    return pl.pallas_call(
        functools.partial(tail_kernel, windows, scale),
        out_shape=(
            jax.ShapeDtypeStruct((window_run, 3), jnp.float32),
            jax.ShapeDtypeStruct((window_run,), jnp.float32),
            jax.ShapeDtypeStruct((window_run,), jnp.float32),
        ),
        in_specs=[smem] * 5,
        out_specs=(smem, smem, smem),
    )(place, parity, inverse_temp, logs, summed)


def solution(mesh):
    return jax.shard_map(
        per_device,
        mesh=mesh,
        in_specs=(P("win", None, "grp"), P("win", "grp"), P("win", "grp"), P(), P(), P(), P()),
        out_specs=(P("win", None), P("win"), P("win")),
        check_vma=False,
    )
```
